256 devices in a mesh: row: 8 (over z), col: 32 (over y, x, core).
Axes of the slice: x: 4, y: 4, z: 8, core: 2. Of those that a mesh axis runs over, the one named last changes fastest.
Arguments:
- node_latent: bfloat16 [262144, 128], P(('row', 'col')), may hold values from -6 to 6
- edge_latent: bfloat16 [1048576, 128], P(('row', 'col')), may hold values from -6 to 6
- senders: int32 [1048576], P(('row', 'col')), may hold values from 0 to 1535
- receivers: int32 [1048576], P(('row', 'col')), may hold values from 0 to 1023
- send_index: int32 [256, 4, 128], P(('row', 'col')), may hold values from 0 to 1023
- context_table: bfloat16 [2048, 128], P(('row', 'col')), may hold values from -6 to 6
- region: int32 [262144], P(('row', 'col')), may hold values from 0 to 2047
- edge_w1: bfloat16 [2, 384, 128], replicated, may hold values from -0.3125 to 0.3125
- edge_w2: bfloat16 [2, 128, 128], replicated, may hold values from -0.5 to 0.5
- edge_bias: float32 [2, 3, 128], replicated, may hold values from -3 to 3
- edge_gain: float32 [2, 128], replicated, may hold values from 0.25 to 1.75
- node_w1: bfloat16 [2, 384, 128], replicated, may hold values from -0.3125 to 0.3125
- node_wg: bfloat16 [2, 128, 128], replicated, may hold values from -0.5 to 0.5
- node_w2: bfloat16 [2, 128, 128], replicated, may hold values from -0.5 to 0.5
- node_bias: float32 [2, 3, 128], replicated, may hold values from -3 to 3
- node_gain: float32 [2, 128], replicated, may hold values from 0.25 to 1.75
Outputs:
- node_out: bfloat16 [262144, 128], P(('row', 'col'))
- edge_out: bfloat16 [1048576, 128], P(('row', 'col'))
The draws below stay inside these ranges and needn't reach their ends.
Inputs may be any that keep to these rules, and one draw needn't show every extreme that they name: senders index the extended table of the edge's own partition: below 1024 its own nodes, then the four received blocks of 128 rows in the order above, below, left, right. receivers are nodes of the edge's own partition. `send_index`: rows of the sending partition's own nodes; repeats may occur.
All inputs are finite; a program needn't handle non-finite values.
Results may differ from the reference program's by a relative error of at most 0.0085.
Values may be sent and summed in bfloat16 or wider, within the bound.
A program may use at most 64 MiB of HBM per device.

```python
import math
import jax
import jax.numpy as jnp
from jax import lax

LATENT = 128
NODES_DEV = 1024
BOUNDARY = 128
LAYERS = 2
EDGES_DEV = 4096
EXTENDED = 1536
PARTS_SIZE = 256
NODES = 262144
EDGES = 1048576
REGIONS = 2048
N_ROW = 8
N_COL = 32


def with_ends(values, key, low, high):
    shape = values.shape
    index_at = [jax.random.randint(jax.random.fold_in(key, axis), (), 0, shape[axis]) for axis in range(len(shape))]
    values = values.at[tuple(index_at)].set(low)
    longest = shape.index(max(shape))
    index_at[longest] = (index_at[longest] + 1) % shape[longest]
    return values.at[tuple(index_at)].set(high)


def steps_of(stream_key, extent, cuts, least, top_value):
    factor_of = 1.0
    for position, shards_of in cuts:
        steps = jax.random.uniform(jax.random.fold_in(jax.random.fold_in(stream_key, 6), position), (shards_of,), jnp.float32, least / len(cuts), top_value / len(cuts))
        factor_of = factor_of * jnp.repeat(jnp.exp(steps), extent[position] // shards_of).reshape((-1,) + (1,) * (len(extent) - 1 - position))
    return factor_of


def bell_draw(stream_key, dims, deviation, reach, cuts=(), dtype=jnp.bfloat16):
    level = steps_of(stream_key, dims, cuts, -0.22, 0.18) if cuts else 1.0
    drawn = jax.random.normal(stream_key, dims, jnp.float32) * deviation * level
    return jnp.minimum(jnp.maximum(drawn, -reach), reach).astype(dtype)


def setup_inputs(seed: int = 0) -> dict:
    splits = jax.random.split(jax.random.key(seed), 17)
    node_latent = bell_draw(splits[0], (NODES, LATENT), 1.0, 6.0, ((0, 256),))
    edge_latent = bell_draw(splits[1], (EDGES, LATENT), 1.0, 6.0, ((0, 256),))
    senders = with_ends(jax.random.randint(splits[2], (EDGES,), 0, EXTENDED), jax.random.fold_in(splits[2], 1), 0, EXTENDED - 1).astype(jnp.int32)
    receivers = with_ends(jax.random.randint(splits[3], (EDGES,), 0, NODES_DEV), jax.random.fold_in(splits[3], 1), 0, NODES_DEV - 1).astype(jnp.int32)
    send_index = with_ends(jax.random.randint(splits[4], (PARTS_SIZE, 4, BOUNDARY), 0, NODES_DEV), jax.random.fold_in(splits[4], 1), 0, NODES_DEV - 1).astype(jnp.int32)
    context_table = bell_draw(splits[5], (REGIONS, LATENT), 1.0, 6.0, ((0, 256),))
    region = with_ends(jax.random.randint(splits[6], (NODES,), 0, REGIONS), jax.random.fold_in(splits[6], 1), 0, REGIONS - 1).astype(jnp.int32)
    edge_w1 = bell_draw(splits[7], (LAYERS, 3 * LATENT, LATENT), (3 * LATENT) ** -0.5, 0.3125)
    edge_w2 = bell_draw(splits[8], (LAYERS, LATENT, LATENT), LATENT ** -0.5, 0.5)
    edge_bias = bell_draw(splits[9], (LAYERS, 3, LATENT), 0.5, 3.0, (), jnp.float32)
    edge_gain = jnp.clip(1.0 + 0.15 * jax.random.normal(splits[10], (LAYERS, LATENT), jnp.float32), 0.25, 1.75)
    node_w1 = bell_draw(splits[11], (LAYERS, 3 * LATENT, LATENT), (3 * LATENT) ** -0.5, 0.3125)
    node_wg = bell_draw(splits[12], (LAYERS, LATENT, LATENT), LATENT ** -0.5, 0.5)
    node_w2 = bell_draw(splits[13], (LAYERS, LATENT, LATENT), LATENT ** -0.5, 0.5)
    node_bias = bell_draw(splits[14], (LAYERS, 3, LATENT), 0.5, 3.0, (), jnp.float32)
    node_gain = jnp.clip(1.0 + 0.15 * jax.random.normal(splits[15], (LAYERS, LATENT), jnp.float32), 0.25, 1.75)
    return dict(node_latent=node_latent, edge_latent=edge_latent, senders=senders, receivers=receivers, send_index=send_index, context_table=context_table, region=region, edge_w1=edge_w1, edge_w2=edge_w2, edge_bias=edge_bias, edge_gain=edge_gain, node_w1=node_w1, node_wg=node_wg, node_w2=node_w2, node_bias=node_bias, node_gain=node_gain)


EPS = 1e-05

def norm_tail(pre, w_out, b_out, gain, shift):
    hidden = jax.nn.relu(pre).astype(jnp.bfloat16)
    y_val = jnp.dot(hidden, w_out, preferred_element_type=jnp.float32) + b_out
    centred = y_val - lax.optimization_barrier(jnp.mean(y_val, axis=-1, keepdims=True))
    spread = lax.optimization_barrier(jnp.mean(centred * centred, axis=-1, keepdims=True))
    return centred * lax.rsqrt(spread + EPS) * gain + shift

def edge_step(extended, edges, senders, receivers, w_in, w_out, bias, gain):
    feats = jnp.concatenate([jnp.take(extended, senders, axis=0), jnp.take(extended, receivers, axis=0), edges], axis=1)
    pre = jnp.dot(feats, w_in, preferred_element_type=jnp.float32) + bias[0]
    return (edges.astype(jnp.float32) + norm_tail(pre, w_out, bias[1], gain, bias[2])).astype(jnp.bfloat16)

def node_step(nodes, new_edges, receivers, context_rows, w_in, w_out, bias, gain, shift_in):
    summed = jax.ops.segment_sum(new_edges.astype(jnp.float32), receivers, num_segments=nodes.shape[0]).astype(jnp.bfloat16)
    feats = jnp.concatenate([nodes, summed, context_rows], axis=1)
    pre = jnp.dot(feats, w_in, preferred_element_type=jnp.float32) + shift_in
    return (nodes.astype(jnp.float32) + norm_tail(pre, w_out, bias[1], gain, bias[2])).astype(jnp.bfloat16)

def pick_rows(nodes, index):
    width = nodes.shape[1]
    return jnp.take(nodes, index.reshape(-1), axis=0).reshape(4, index.shape[1], width)

def with_halo(nodes, send_index):
    sent = jax.vmap(jax.vmap(pick_rows))(nodes, send_index)
    zero_row = jnp.zeros_like(sent[:1, :, 0])
    from_above = jnp.concatenate([zero_row, sent[:-1, :, 0]], axis=0)
    from_below = jnp.concatenate([sent[1:, :, 1], zero_row], axis=0)
    zero_col = jnp.zeros_like(sent[:, :1, 2])
    from_left = jnp.concatenate([zero_col, sent[:, :-1, 2]], axis=1)
    from_right = jnp.concatenate([sent[:, 1:, 3], zero_col], axis=1)
    return jnp.concatenate([nodes, from_above, from_below, from_left, from_right], axis=2)

def reference(node_latent, edge_latent, senders, receivers, send_index, context_table, region, edge_w1, edge_w2, edge_bias, edge_gain, node_w1, node_wg, node_w2, node_bias, node_gain):
    width = node_latent.shape[1]
    pooled = lax.optimization_barrier(jnp.sum(node_latent.astype(jnp.float32), axis=0)) / math.sqrt(NODES)
    nodes = node_latent.reshape(N_ROW, N_COL, NODES_DEV, width)
    edges = edge_latent.reshape(PARTS_SIZE, EDGES_DEV, width)
    sender_rows = senders.reshape(PARTS_SIZE, EDGES_DEV)
    receiver_rows = receivers.reshape(PARTS_SIZE, EDGES_DEV)
    index = send_index.reshape(N_ROW, N_COL, 4, BOUNDARY)
    context_rows = jnp.take(context_table, region, axis=0).reshape(PARTS_SIZE, NODES_DEV, width)
    for layer in range(LAYERS):
        extended = with_halo(nodes, index).reshape(PARTS_SIZE, EXTENDED, width)
        flat = nodes.reshape(PARTS_SIZE, NODES_DEV, width)
        shift_in = node_bias[layer, 0] + jnp.dot(pooled, node_wg[layer].astype(jnp.float32), precision=lax.Precision.HIGHEST)

        def one_part(items, layer=layer, shift_in=shift_in):
            ext_p, edges_p, send_p, recv_p, nodes_p, ctx_p = items
            new_edges = edge_step(ext_p, edges_p, send_p, recv_p, edge_w1[layer], edge_w2[layer], edge_bias[layer], edge_gain[layer])
            new_nodes = node_step(nodes_p, new_edges, recv_p, ctx_p, node_w1[layer], node_w2[layer], node_bias[layer], node_gain[layer], shift_in)
            return (new_edges, new_nodes)
        edges, flat = lax.map(one_part, (extended, edges, sender_rows, receiver_rows, flat, context_rows))
        nodes = flat.reshape(N_ROW, N_COL, NODES_DEV, width)
    return (nodes.reshape(NODES, width), edges.reshape(EDGES, width))
```

```python
import functools
import math

import jax
import jax.numpy as jnp
from jax import lax
from jax.experimental import pallas as pl
from jax.experimental.pallas import tpu as pltpu
from jax.sharding import PartitionSpec as P

LAYERS = 2
EPS = 1e-05
LANES = 128
BLOCK = 512
TILE = 256
CORES = 2
F32 = jnp.float32
BF16 = jnp.bfloat16
MESH = pl.DeviceIdType.MESH


def mm(a, b):
    return jnp.dot(a, b, preferred_element_type=F32)


def iota(axis):
    return lax.broadcasted_iota(jnp.int32, (LANES, LANES), axis)


def as_column(row):
    return jnp.transpose(jnp.broadcast_to(row, (LANES, LANES)))


def hot(mask):
    return jnp.where(mask, 1.0, 0.0).astype(BF16)


def pick_parts(lane, group, axis, parts):
    base = hot(lane == iota(axis))
    group = group.astype(F32).astype(BF16)
    zero = jnp.zeros_like(base)
    return [jnp.where(group == jnp.asarray(part, BF16), base, zero) for part in range(parts)]


def pick_rows(lane, group, parts):
    return jnp.concatenate(pick_parts(lane, group, 1, parts), axis=1)


def pick_tiles(index, parts):
    group = ((index >> 9) << 1) + ((index >> 7) & 1)
    return pick_rows(index & (LANES - 1), group, parts)


def centre(values):
    values = values.astype(F32)
    return values - jnp.mean(values, axis=-1, keepdims=True)


def twice(weight):
    zero = jnp.zeros_like(weight)
    top = jnp.concatenate([weight, zero], axis=1)
    return jnp.concatenate([top, jnp.concatenate([zero, weight], axis=1)], axis=0)


def norm(centred, gain, shift):
    spread = jnp.mean(centred * centred, axis=-1, keepdims=True)
    return centred * lax.rsqrt(spread + EPS) * gain + shift


def kernel(
    n_row,
    n_col,
    rest,
    barrier,
    place_of,
    node_ref,
    edge_ref,
    send_ref,
    recv_ref,
    index_ref,
    ctx_ref,
    region_ref,
    ew1,
    ew2,
    eb,
    eg,
    nw1,
    nwg,
    nw2,
    nb,
    ng,
    node_out,
    edge_out,
    hot_send,
    hot_recv,
    hot_sum,
    side_send,
    side_recv,
    hot_index,
    side_index,
    hot_ctx,
    picked,
    ctx_all,
    pool_row,
    pool_chip,
    pool_core,
    from_ext,
    from_own,
    sums,
    ctx_part,
    parts,
    edge_sem,
    halo_send_sem,
    halo_recv_sem,
    row_send_sem,
    row_recv_sem,
    col_send_sem,
    col_recv_sem,
    core_send_sem,
    core_recv_sem,
):
    my_row, my_col, my_chip, my_core, partner = place_of()
    nodes, width = node_ref.shape
    edges = edge_ref.shape[0]
    count = index_ref.shape[1]
    ext = nodes + 4 * count
    half_ext, half_own = ext // 2, nodes // 2
    ctx_rows = ctx_ref.shape[0]
    n_chip = n_col // CORES
    half_regions = n_chip * n_row * ctx_rows
    edge_in = pltpu.make_async_copy(edge_ref, edge_out, edge_sem)
    edge_in.start()
    per_block = 2 * BLOCK // LANES

    ctx_all[my_core, my_chip, my_row] = ctx_ref[...]
    pool_row[my_row] = jnp.sum(node_ref[...].astype(F32).reshape(nodes // 8, 8, width), axis=0)

    def fill_send(layer, now):
        both = mm(now[...], ew1[layer, :width]).astype(BF16)
        for t in range(nodes // (2 * TILE)):
            for side in range(2):
                part = both[(2 * t + side) * TILE : (2 * t + side + 1) * TILE]
                from_ext[layer, t * TILE : (t + 1) * TILE, side * width : (side + 1) * width] = part

    def fill_recv(layer, now):
        both = mm(now[...], ew1[layer, width : 2 * width]).astype(BF16)
        from_own[:, :width] = both[:half_own]
        from_own[:, width:] = both[half_own:]

    def pick(layer):
        both = mm(hot_index[...], from_ext[layer, :half_own])
        picked[layer] = jnp.where(side_index[...] > 0, both[:, width:], both[:, :width]).astype(BF16)

    for side in range(4):
        rows = slice(side * count, (side + 1) * count)
        column = as_column(index_ref[side : side + 1, :])
        hot_index[rows, :] = pick_tiles(column, half_own // LANES)
        side_index[rows, :] = (column >> 8) & 1
    fill_send(0, node_ref)
    pick(0)

    pl.semaphore_wait(barrier, n_row + n_chip)

    moves = (
        (my_row + 1, my_col, my_row < n_row - 1, my_row > 0),
        (my_row - 1, my_col, my_row > 0, my_row < n_row - 1),
        (my_row, my_col + 1, my_col < n_col - 1, my_col > 0),
        (my_row, my_col - 1, my_col > 0, my_col < n_col - 1),
    )

    def halo_place(side):
        rows = slice(half_own + side % 2 * count, half_own + (side % 2 + 1) * count)
        return rows, slice(side // 2 * width, (side // 2 + 1) * width)

    def halo_copy(layer, side):
        to_row, to_col = moves[side][:2]
        rows, lanes = halo_place(side)
        return pltpu.make_async_remote_copy(
            src_ref=picked.at[layer, side * count : (side + 1) * count],
            dst_ref=from_ext.at[layer, rows, lanes],
            send_sem=halo_send_sem.at[layer, side],
            recv_sem=halo_recv_sem.at[layer, side],
            device_id=(to_row, to_col),
            device_id_type=MESH,
        )

    def halo_start(layer):
        for side in range(4):

            @pl.when(moves[side][2])
            def _(side=side):
                halo_copy(layer, side).start()

    def halo_wait(layer):
        for side in range(4):

            @pl.when(moves[side][3])
            def _(side=side):
                halo_copy(layer, side).wait_recv()

            @pl.when(jnp.logical_not(moves[side][3]))
            def _(side=side):
                rows, lanes = halo_place(side)
                from_ext[layer, rows, lanes] = jnp.zeros((count, width), BF16)

    def send(src, send_sem, recv_sem, device):
        return pltpu.make_async_remote_copy(
            src_ref=src,
            dst_ref=src,
            send_sem=send_sem,
            recv_sem=recv_sem,
            device_id=device,
            device_id_type=MESH,
        )

    def row_copies(step, owner):
        device = (lax.rem(my_row + step, n_row), my_col)
        refs = (pool_row.at[owner], ctx_all.at[my_core, my_chip, owner])
        return [
            send(ref, row_send_sem.at[k, step - 1], row_recv_sem.at[k, step - 1], device)
            for k, ref in enumerate(refs)
        ]

    def col_copies(step, owner):
        device = (my_row, lax.rem(my_chip + step, n_chip) * CORES + my_core)
        refs = (pool_chip.at[owner], ctx_all.at[my_core, owner])
        return [
            send(ref, col_send_sem.at[k, step - 1], col_recv_sem.at[k, step - 1], device)
            for k, ref in enumerate(refs)
        ]

    def core_copies(owner):
        refs = (pool_core.at[owner], ctx_all.at[owner])
        return [
            send(ref, core_send_sem.at[k], core_recv_sem.at[k], (my_row, partner))
            for k, ref in enumerate(refs)
        ]

    for step in range(1, n_row):
        for copy in row_copies(step, my_row):
            copy.start()
    halo_start(0)
    for copy in rest:
        copy.wait()

    def prepare(block, carry):
        for sub in range(per_block):
            line = block * per_block + sub
            send_row = send_ref[pl.ds(line, 1), :]
            recv_row = recv_ref[pl.ds(line, 1), :]
            rows = pl.ds(pl.multiple_of(line * LANES, LANES), LANES)
            both = as_column(send_row + (recv_row << 16))
            send, recv = both & 0xFFFF, both >> 16
            side_send[rows, :] = (send >> 8) & 1
            recv_high = (recv >= half_own).astype(jnp.int32)
            side_recv[rows, :] = recv_high
            hot_send[rows, :] = pick_tiles(send, half_ext // LANES)
            recv -= recv_high * half_own
            hot_recv[rows, :] = pick_rows(recv & (LANES - 1), recv >> 7, half_own // LANES)
            recv_low = recv_row - (recv_row >= half_own).astype(jnp.int32) * half_own
            recv_low = jnp.broadcast_to(recv_low, (LANES, LANES))
            recv_parts = pick_parts(recv_low & (LANES - 1), recv_low >> 7, 0, half_own // LANES)
            for part, value in enumerate(recv_parts):
                hot_sum[
                    block, part * LANES : (part + 1) * LANES, sub * LANES : (sub + 1) * LANES
                ] = value
        return carry

    lax.fori_loop(0, edges // (2 * BLOCK), prepare, 0)

    for step in range(1, n_row):
        for copy in row_copies(step, lax.rem(my_row + n_row - step, n_row)):
            copy.wait_recv()
    pool_chip[my_chip] = jnp.sum(pool_row[...], axis=0)
    for step in range(1, n_chip):
        for copy in col_copies(step, my_chip):
            copy.start()

    def regions_line(line, carry):
        region = as_column(region_ref[pl.ds(line, 1), :])
        chip = (region >> 4) & (n_chip - 1)
        far = ((region >> 3) & 1) ^ my_core
        spot = (chip * n_row + (region >> 8)) * ctx_rows + (region & 7) + far * half_regions
        rows = pl.ds(pl.multiple_of(line * LANES, LANES), LANES)
        hot_ctx[rows, :] = pick_rows(spot & (LANES - 1), spot >> 7, CORES * half_regions // LANES)
        return carry

    lax.fori_loop(0, nodes // LANES, regions_line, 0)

    def edge_phase(layer):
        sums[...] = jnp.zeros_like(sums)
        parts[...] = jnp.zeros_like(parts)
        w_edge = twice(ew1[layer, 2 * width :])
        w_out = twice(centre(ew2[layer]).astype(BF16))
        b_in = eb[0, layer : layer + 1]
        b_out = centre(eb[1, layer : layer + 1])

        def scatter(pair):
            sums[...] += mm(hot_sum[pair], parts[...])

        def body(pair, carry):
            blocks = [
                pl.ds(pl.multiple_of((2 * pair + half) * BLOCK, BLOCK), BLOCK) for half in range(2)
            ]
            old = [edge_out[rows, :] for rows in blocks]
            by_edge = mm(jnp.concatenate(old, axis=1), w_edge)
            by_send = [mm(hot_send[rows, :], from_ext[layer]) for rows in blocks]
            by_recv = [mm(hot_recv[rows, :], from_own[...]) for rows in blocks]
            scatter(jnp.maximum(pair - 1, 0))
            hidden = []
            for half, rows in enumerate(blocks):
                pre = by_edge[:, half * width : (half + 1) * width] + b_in
                pre += jnp.where(
                    side_send[rows, :] > 0, by_send[half][:, width:], by_send[half][:, :width]
                )
                pre += jnp.where(
                    side_recv[rows, :] > 0, by_recv[half][:, width:], by_recv[half][:, :width]
                )
                hidden.append(jnp.maximum(pre, 0.0).astype(BF16))
            y_val = mm(jnp.concatenate(hidden, axis=1), w_out)
            for half, rows in enumerate(blocks):
                centred = y_val[:, half * width : (half + 1) * width] + b_out
                new = old[half].astype(F32)
                new += norm(centred, eg[layer : layer + 1], eb[2, layer : layer + 1])
                edge_out[rows, :] = new.astype(BF16)
                high = side_recv[rows, :] > 0
                place = slice(half * BLOCK, (half + 1) * BLOCK)
                parts[place, :width] = jnp.where(high, 0.0, new).astype(BF16)
                parts[place, width:] = jnp.where(high, new, 0.0).astype(BF16)
            return carry

        pairs = edges // (2 * BLOCK)
        lax.fori_loop(0, pairs, body, 0)
        scatter(pairs - 1)

    def node_phase(layer, now, shift_in):
        summed = jnp.concatenate([sums[:, :width], sums[:, width:]], axis=0).astype(BF16)
        feats = jnp.concatenate([now[...], summed], axis=1)
        pre = mm(feats, nw1[layer, : 2 * width]) + shift_in
        pre += ctx_part[:, layer * width : (layer + 1) * width]
        hidden = jnp.maximum(pre, 0.0).astype(BF16)
        centred = mm(hidden, centre(nw2[layer]).astype(BF16)) + centre(nb[1, layer : layer + 1])
        new = now[...].astype(F32)
        new += norm(centred, ng[layer : layer + 1], nb[2, layer : layer + 1])
        node_out[...] = new.astype(BF16)

    fill_recv(0, node_ref)
    halo_wait(0)
    edge_in.wait()
    edge_phase(0)

    for step in range(1, n_chip):
        for copy in col_copies(step, lax.rem(my_chip + n_chip - step, n_chip)):
            copy.wait_recv()
    pool_core[my_core] = jnp.sum(pool_chip[...], axis=0)
    for copy in core_copies(my_core):
        copy.start()
    w_pair = jnp.concatenate([nw1[l, 2 * width :] for l in range(LAYERS)], axis=1)

    def context_half(core, place):
        rows = ctx_all[core].astype(F32).reshape(half_regions, width).astype(BF16)
        projected = mm(rows, w_pair).astype(BF16)
        return mm(hot_ctx[:, place * half_regions : (place + 1) * half_regions], projected)

    ctx_part[...] = context_half(my_core, 0)
    for copy in core_copies(1 - my_core):
        copy.wait_recv()
    ctx_part[...] += context_half(1 - my_core, 1)
    pooled = jnp.sum(pool_core[0] + pool_core[1], axis=0, keepdims=True)
    pooled = pooled / math.sqrt(nodes * n_row * n_col)

    def shift_of(layer):
        weight = nwg[layer].astype(F32)
        term = jnp.dot(
            pooled, weight, precision=lax.Precision.HIGHEST, preferred_element_type=F32
        )
        return nb[0, layer : layer + 1] + term

    node_phase(0, node_ref, shift_of(0))

    fill_send(1, node_out)
    pick(1)
    halo_start(1)
    fill_recv(1, node_out)
    last_shift = shift_of(1)
    halo_wait(1)
    edge_phase(1)
    node_phase(1, node_out, last_shift)

    for layer in range(LAYERS):
        for side in range(4):

            @pl.when(moves[side][2])
            def _(layer=layer, side=side):
                halo_copy(layer, side).wait_send()

    for step in range(1, n_row):
        for copy in row_copies(step, my_row):
            copy.wait_send()
    for step in range(1, n_chip):
        for copy in col_copies(step, my_chip):
            copy.wait_send()
    for copy in core_copies(my_core):
        copy.wait_send()


EARLY = (0, 4, 5, 7)


def entry(n_row, n_col, count, *refs):
    given, others = refs[:count], list(refs[count : -count])
    held, copy_sem = refs[-count:-1], refs[-1]
    places = list(held)
    places.insert(1, None)
    copies = {
        k: pltpu.make_async_copy(given[k], places[k], copy_sem.at[k])
        for k in range(count)
        if k != 1
    }
    order = EARLY + tuple(k for k in copies if k not in EARLY)
    for k in order:
        copies[k].start()

    def place_of():
        my_row, my_col = lax.axis_index("row"), lax.axis_index("col")
        my_chip, my_core = my_col // CORES, lax.rem(my_col, CORES)
        return my_row, my_col, my_chip, my_core, my_chip * CORES + 1 - my_core

    my_row, my_col, my_chip, my_core, partner = place_of()
    n_chip = n_col // CORES
    barrier = pltpu.get_barrier_semaphore()
    beside = lax.rem(my_col + CORES * my_core - 1 + n_col, n_col)
    peers = [(lax.rem(my_row + step, n_row), my_col) for step in range(1, n_row)]
    peers += [
        (my_row, lax.rem(my_chip + step, n_chip) * CORES + my_core) for step in range(1, n_chip)
    ]
    for peer in peers + [(my_row, partner), (my_row, beside)]:
        pl.semaphore_signal(barrier, inc=1, device_id=peer, device_id_type=MESH)
    for k in EARLY:
        copies[k].wait()
    places[1] = given[1]
    rest = [copies[k] for k in order if k not in EARLY]
    kernel(n_row, n_col, rest, barrier, place_of, *places, *others)


def local(n_row, n_col, *args):
    node, edge, send, recv, index, ctx, region = args[:7]
    nodes, width = node.shape
    edges = edge.shape[0]
    count = index.shape[2]
    half_ext, half_own = (nodes + 4 * count) // 2, nodes // 2
    n_chip = n_col // CORES
    vmem = pl.BlockSpec(memory_space=pltpu.VMEM)
    dma = pltpu.SemaphoreType.DMA
    operands = (
        node,
        edge,
        send.reshape(edges // LANES, LANES),
        recv.reshape(edges // LANES, LANES),
        index.reshape(4, count),
        ctx,
        region.reshape(nodes // LANES, LANES),
    ) + args[7:]
    operands = tuple(
        jnp.transpose(x, (1, 0, 2)) if x.shape == (LAYERS, 3, width) else x for x in operands
    )
    operands = tuple(pltpu.with_memory_space_constraint(x, pltpu.HBM) for x in operands)
    return pl.pallas_call(
        functools.partial(entry, n_row, n_col, len(operands)),
        out_shape=(
            jax.ShapeDtypeStruct(node.shape, BF16),
            jax.ShapeDtypeStruct(edge.shape, BF16),
        ),
        in_specs=[pl.BlockSpec(memory_space=pltpu.HBM)] * len(operands),
        out_specs=(vmem, vmem),
        scratch_shapes=[
            pltpu.VMEM((edges, half_ext), BF16),
            pltpu.VMEM((edges, half_own), BF16),
            pltpu.VMEM((edges // (2 * BLOCK), half_own, 2 * BLOCK), BF16),
            pltpu.VMEM((edges, width), jnp.int32),
            pltpu.VMEM((edges, width), jnp.int32),
            pltpu.VMEM((4 * count, half_own), BF16),
            pltpu.VMEM((4 * count, width), jnp.int32),
            pltpu.VMEM((nodes, n_row * n_col * ctx.shape[0]), BF16),
            pltpu.VMEM((LAYERS, 4 * count, width), BF16),
            pltpu.VMEM((CORES, n_chip, n_row, *ctx.shape), BF16),
            pltpu.VMEM((n_row, 8, width), F32),
            pltpu.VMEM((n_chip, 8, width), F32),
            pltpu.VMEM((CORES, 8, width), F32),
            pltpu.VMEM((LAYERS, half_ext, 2 * width), BF16),
            pltpu.VMEM((half_own, 2 * width), BF16),
            pltpu.VMEM((half_own, 2 * width), F32),
            pltpu.VMEM((nodes, LAYERS * width), F32),
            pltpu.VMEM((2 * BLOCK, 2 * width), BF16),
            dma(()),
            dma((LAYERS, 4)),
            dma((LAYERS, 4)),
            dma((2, n_row - 1)),
            dma((2, n_row - 1)),
            dma((2, n_chip - 1)),
            dma((2, n_chip - 1)),
            dma((2,)),
            dma((2,)),
        ]
        + [pltpu.VMEM(x.shape, x.dtype) for k, x in enumerate(operands) if k != 1]
        + [dma((len(operands),))],
        compiler_params=pltpu.CompilerParams(
            collective_id=0, has_side_effects=True, vmem_limit_bytes=36 * 1024 * 1024
        ),
        name="mesh_steps",
    )(*operands)


def solution(mesh):
    both = ("row", "col")
    split = (P(both, None), P(both, None), P(both), P(both), P(both, None, None), P(both, None), P(both))
    return jax.shard_map(
        functools.partial(local, mesh.shape["row"], mesh.shape["col"]),
        mesh=mesh,
        in_specs=split + (P(),) * 9,
        out_specs=(P(both, None), P(both, None)),
        check_vma=False,
    )
```
